32 devices in a mesh: pipe: 2 (over core), dp: 4 (over z), mp: 4 (over y, x).
Axes of the slice: x: 2, y: 2, z: 4, core: 2. Of those that a mesh axis runs over, the one named last changes fastest.
Arguments:
- hidden_states: bfloat16 [16, 64, 4096], P('dp'), may hold values from -6 to 6
- up_weight: bfloat16 [2, 4096, 7168], P('pipe', 'dp', 'mp'), may hold values from -0.09375 to 0.09375
- down_weight: bfloat16 [2, 7168, 4096], P('pipe', 'mp', 'dp'), may hold values from -0.0625 to 0.0625
- layer_gain: float32 [2, 4096], P('pipe'), may hold values from 0.5 to 1.5
- final_gain: float32 [4096], replicated, may hold values from 0.5 to 1.5
- unembedding: bfloat16 [32768, 4096], P(('pipe', 'mp')), may hold values from -32 to 32
- target_ids: int32 [16, 64], P('dp'), may hold values from 0 to 32767
- response_masks: int32 [16, 64], P('dp'), may hold values from 0 to 1, as said below
- anchor_logps: float32 [16, 64], P('dp'), may hold values from -14 to -10
- pairing: int32 [4, 4], P('dp'), may hold values from 0 to 3, each once within a row
Outputs:
- token_logps: float32 [16, 64], P('dp')
- seq_logps: float32 [16], P('dp')
- pair_losses: float32 [8], P('dp')
The draws below stay inside these ranges and needn't reach their ends.
Inputs may be any that keep to these rules, and one draw needn't show every extreme that they name: response_masks is 1 on one unbroken run of at least one position per sequence, starting at or after position 8, and 0 elsewhere.
All inputs are finite; a program needn't handle non-finite values.
Results may differ from the reference program's by a relative error of at most 0.0075.
Values may be sent and summed in bfloat16 or wider, within the bound.
No kernel may reach another device: no remote copies, remote signals or barrier semaphores. Data moves between devices by JAX's collectives and lax.ppermute only.
A program may use at most 192 MiB of HBM per device.

```python
import math
import jax
import jax.numpy as jnp
import numpy as np
from jax import lax

D = 4096
VOCAB = 32768
FF = 7168
LEN = 64
SEQ_DEV = 4
SEQ_MB = 1
MICRO = 4
GROUPS = 4
SEQS = 16
PAIRS = 8
SECTIONS = 2


def draw_unembedding(key, part):
    values = jax.random.normal(key, (VOCAB, D), jnp.float32) * (2.0 * D ** (-0.5))
    values = jnp.clip(values, -12.0 * D ** (-0.5), 12.0 * D ** (-0.5))
    return values.astype(jnp.bfloat16)


def draw_response_masks(key, part):
    first_key, second_key = jax.random.split(key)
    starts = jax.random.randint(first_key, (SEQS, 1), LEN // 8, LEN // 2)
    spread = jax.random.randint(second_key, (SEQS, 1), 0, 1 << 20)
    spans = 1 + spread % (LEN - starts)
    positions = jnp.arange(LEN, dtype=jnp.int32)[None, :]
    return ((positions >= starts) & (positions < starts + spans)).astype(jnp.int32)


def set_ends(array, key, low, largest):
    spot = [jax.random.randint(jax.random.fold_in(key, axis), (), 0, length) for axis, length in enumerate(array.shape)]
    main_axis = array.shape.index(max(array.shape))
    next_to = spot[:main_axis] + [(spot[main_axis] + 1) % array.shape[main_axis]] + spot[main_axis + 1:]
    return array.at[tuple(spot)].set(low).at[tuple(next_to)].set(largest)


def steps_of(key, dims, cuts, low, largest):
    def one(axis_at, parts):
        heights = jax.random.uniform(jax.random.fold_in(jax.random.fold_in(key, 6), axis_at), (parts,), jnp.float32, low / len(cuts), largest / len(cuts))
        return jnp.repeat(jnp.exp(heights), dims[axis_at] // parts).reshape((-1,) + (1,) * (len(dims) - axis_at - 1))

    gain = one(*cuts[0])
    for cut in cuts[1:]:
        gain = gain * one(*cut)
    return gain


def rank_table(count, lean):
    portions = [(1 << 20) // math.isqrt(grade ** lean) + 1 for grade in range(1, count + 1)]
    scale = 1 + sum(portions) // (1 << 30)
    return np.cumsum(np.array([max(1, weight // scale) for weight in portions]))


def ranked_ids(rng, dims, amount, skew):
    table = rank_table(amount, skew)
    lot = jax.random.randint(jax.random.fold_in(rng, 1), dims, 0, int(table[amount - 1]))
    standing = jnp.searchsorted(jnp.asarray(table, jnp.int32), lot, side="right")
    return jax.random.permutation(jax.random.fold_in(rng, 2), amount)[standing].astype(jnp.int32)


def normal_values(own_key, dims, width, most, shards=(), kind=jnp.bfloat16):
    values = jax.random.normal(own_key, dims, jnp.float32) * width
    if len(shards) > 0:
        values = steps_of(own_key, dims, shards, -0.22, 0.18) * values
    return jnp.clip(values, min=-most, max=most).astype(kind)


def setup_inputs(seed: int = 0) -> dict:
    key_list = jax.random.split(jax.random.key(seed), 11)
    hidden_states = normal_values(key_list[0], (SEQS, LEN, D), 1.0, 6.0, ((0, 4),))
    up_weight = normal_values(key_list[1], (SECTIONS, D, FF), D ** -0.5, 0.09375, ((0, 2), (1, 4), (2, 4)))
    down_weight = normal_values(key_list[2], (SECTIONS, FF, D), FF ** -0.5, 0.0625, ((0, 2), (1, 4), (2, 4)))
    layer_gain = jnp.clip(1.0 + 0.1 * jax.random.normal(key_list[3], (SECTIONS, D), jnp.float32), 0.5, 1.5)
    final_gain = jnp.clip(1.0 + 0.1 * jax.random.normal(key_list[4], (D,), jnp.float32), 0.5, 1.5)
    unembedding = draw_unembedding(jax.random.fold_in(key_list[10], 71), 0)
    target_ids = set_ends(ranked_ids(key_list[6], (SEQS, LEN), VOCAB, 2), jax.random.fold_in(key_list[6], 3), 0, VOCAB - 1).astype(jnp.int32)
    response_masks = draw_response_masks(jax.random.fold_in(key_list[10], 71), 0)
    anchor_logps = jnp.clip(-14.0 + 4.0 * jax.random.uniform(key_list[8], (SEQS, LEN), jnp.float32) ** steps_of(key_list[8], (SEQS, LEN), ((0, 4),), -0.2, 0.2), -14.0, -10.0)
    pairing = jax.vmap(lambda own: jax.random.permutation(own, SEQ_DEV))(jax.random.split(key_list[9], GROUPS)).reshape((GROUPS, SEQ_DEV)).astype(jnp.int32)
    return dict(hidden_states=hidden_states, up_weight=up_weight, down_weight=down_weight, layer_gain=layer_gain, final_gain=final_gain, unembedding=unembedding, target_ids=target_ids, response_masks=response_masks, anchor_logps=anchor_logps, pairing=pairing)


epsilon = 1e-05
ipo_tau = 0.5

def rms_scale(values, gain_row):
    mean_square = lax.optimization_barrier(jnp.mean(values * values, axis=-1, keepdims=True))
    return values * lax.rsqrt(mean_square + epsilon) * gain_row.astype(jnp.float32)

def section_layer(states, gain_row, up_matrix, down_matrix):
    wide_states = states.astype(jnp.float32)
    normed = rms_scale(wide_states, gain_row).astype(jnp.bfloat16)
    active = jax.nn.silu(jnp.dot(normed, up_matrix, preferred_element_type=jnp.float32)).astype(jnp.bfloat16)
    summed = wide_states + jnp.dot(active, down_matrix, preferred_element_type=jnp.float32)
    return summed.astype(jnp.bfloat16)

def token_scores(finals, final_gain, unembedding, wanted_ids):
    normed = rms_scale(finals.astype(jnp.float32), final_gain).astype(jnp.bfloat16)
    logits = jnp.dot(normed, unembedding.T, preferred_element_type=jnp.float32)
    top_value = lax.optimization_barrier(jnp.max(logits, axis=1, keepdims=True))
    log_total = top_value[:, 0] + jnp.log(lax.optimization_barrier(jnp.sum(jnp.exp(logits - top_value), axis=1)))
    picked = jnp.take_along_axis(logits, wanted_ids[:, None], axis=1)[:, 0]
    return picked - log_total

def reference(hidden_states, up_weight, down_weight, layer_gain, final_gain, unembedding, target_ids, response_masks, anchor_logps, pairing):

    def one_group(group_items):
        states, wanted_ids = group_items
        flat_states = states.reshape(SEQ_DEV * LEN, D)
        for section_index in range(SECTIONS):
            flat_states = section_layer(flat_states, layer_gain[section_index], up_weight[section_index], down_weight[section_index])
        return token_scores(flat_states, final_gain, unembedding, wanted_ids.reshape(SEQ_DEV * LEN)).reshape(SEQ_DEV, LEN)
    token_logps = lax.map(one_group, (hidden_states.reshape(GROUPS, SEQ_DEV, LEN, D), target_ids.reshape(GROUPS, SEQ_DEV, LEN)))
    token_logps = token_logps.reshape(SEQS, LEN)
    mask_values = response_masks.astype(jnp.float32)
    counts = lax.optimization_barrier(jnp.sum(mask_values.reshape(GROUPS, MICRO, SEQ_MB * LEN), axis=(0, 2)))
    mean_length = counts / (GROUPS * SEQ_MB)
    divisor = jnp.tile(jnp.repeat(mean_length, SEQ_MB), GROUPS)
    policy = lax.optimization_barrier(jnp.sum(mask_values * token_logps, axis=1)) / divisor
    anchor = lax.optimization_barrier(jnp.sum(mask_values * anchor_logps, axis=1)) / divisor
    log_gaps = (policy - anchor).reshape(GROUPS, SEQ_DEV)
    chosen = jnp.take_along_axis(log_gaps, pairing[:, 0::2], axis=1)
    rejected = jnp.take_along_axis(log_gaps, pairing[:, 1::2], axis=1)
    losses = (chosen - rejected - 0.5 / ipo_tau) ** 2
    return (token_logps, policy, losses.reshape(PAIRS))
```

```python
import jax
import jax.numpy as jnp
from jax import lax
from jax.sharding import PartitionSpec as P


epsilon = 1e-05
ipo_tau = 0.5


def shift(value, axis, steps):
    count = lax.axis_size(axis)
    if steps % count == 0:
        return value
    return lax.ppermute(value, axis, [(i, (i + steps) % count) for i in range(count)])


def swap(value, axis, mask):
    if mask == 0:
        return value
    count = lax.axis_size(axis)
    return lax.ppermute(value, axis, [(i, i ^ mask) for i in range(count)])


def flip_by(value, axis, index, count):
    bit = 1
    while bit < count:
        shape = value.shape
        parts = value.reshape(shape[:axis] + (count // (2 * bit), 2, bit) + shape[axis + 1 :])
        turned = jnp.flip(parts, axis + 1)
        value = jnp.where((index & bit) != 0, turned, parts).reshape(shape)
        bit *= 2
    return value


def shards(
    hidden_states,
    up_weight,
    down_weight,
    layer_gain,
    final_gain,
    unembedding,
    target_ids,
    response_masks,
    anchor_logps,
    pairing,
):
    seq_count, length, width = hidden_states.shape
    n_dp, n_mp, n_pipe = lax.axis_size("dp"), lax.axis_size("mp"), lax.axis_size("pipe")
    dp, mp, pipe = lax.axis_index("dp"), lax.axis_index("mp"), lax.axis_index("pipe")
    rows = seq_count * length // (n_pipe * n_mp)
    cols = up_weight.shape[1]
    f32, bf16 = jnp.float32, jnp.bfloat16

    mask_values = response_masks.astype(f32)
    local_counts = jnp.sum(mask_values, axis=1)
    counts = local_counts
    for step in range(1, n_dp):
        counts = counts + shift(local_counts, "dp", step)

    def both(own):
        other = swap(own, "pipe", 1)
        first = jnp.where(pipe == 0, own, other)
        second = jnp.where(pipe == 0, other, own)
        return first, second

    gain_own = lax.dynamic_slice_in_dim(layer_gain[0], dp * cols, cols, 0)
    ups = lax.optimization_barrier(both(up_weight[0]))
    downs = lax.optimization_barrier(both(down_weight[0]))
    gains = both(gain_own)

    x_core = lax.dynamic_index_in_dim(
        hidden_states.reshape(n_pipe, n_mp, rows, width), pipe, 0, keepdims=False
    )
    x_mine = lax.dynamic_index_in_dim(x_core, mp, 0, keepdims=False)
    x_wide = x_core.astype(f32)
    mean_square = jnp.mean(x_wide * x_wide, axis=-1)
    row_scale = flip_by(lax.rsqrt(mean_square + epsilon), 0, mp, n_mp).reshape(-1)

    blocks = []
    for step in range(n_dp):
        start = ((dp + step) % n_dp) * cols
        blocks.append(shift(lax.dynamic_slice_in_dim(x_mine, start, cols, 1), "dp", step))

    def gather_mp(block):
        return jnp.concatenate([swap(block, "mp", k) for k in range(n_mp)], axis=0)

    order = list(range(1, n_dp)) + [0]

    def section(blocks, gathered, row_scale, gain, up, down):
        partials = {}
        for t in order:
            scaled = (gathered[t].astype(f32) * gain).astype(bf16)
            partials[t] = lax.optimization_barrier(jnp.dot(scaled, up, preferred_element_type=f32))
        total = partials[order[0]]
        for t in order[1:]:
            total = shift(total.astype(bf16), "dp", 1).astype(f32) + partials[t]
        current = jax.nn.silu(total * row_scale[:, None]).astype(bf16)
        results = []
        for t in range(n_dp):
            if t > 0:
                current = shift(current, "dp", 1)
            out = jnp.dot(current, down, preferred_element_type=f32).reshape(n_mp, rows, cols)
            summed = blocks[t].astype(f32) + out[0]
            for k in range(1, n_mp):
                summed = summed + swap(out[k].astype(bf16), "mp", k).astype(f32)
            results.append(summed.astype(bf16))
        return results

    gathered = [gather_mp(block) for block in blocks]
    blocks = section(blocks, gathered, row_scale, gains[0], ups[0], downs[0])

    gathered = [gather_mp(block) for block in blocks]
    square_sum = 0.0
    for t in range(n_dp):
        wide = gathered[t].astype(f32)
        square_sum = square_sum + shift(jnp.sum(wide * wide, axis=-1), "dp", -t)
    row_scale = lax.rsqrt(square_sum / width + epsilon)
    blocks = section(blocks, gathered, row_scale, gains[1], ups[1], downs[1])

    home = [shift(blocks[t], "dp", -t) for t in range(n_dp)]
    doubled = jnp.concatenate([jnp.stack(home), jnp.stack(home)], axis=0)
    placed = lax.dynamic_slice_in_dim(doubled, (n_dp - dp) % n_dp, n_dp, 0)
    finals = jnp.transpose(placed, (1, 0, 2)).reshape(rows, width).astype(f32)
    mean_square = jnp.mean(finals * finals, axis=-1, keepdims=True)
    normed = (finals * lax.rsqrt(mean_square + epsilon) * final_gain).astype(bf16)
    near = gather_mp(normed)
    everyone = jnp.concatenate([near, swap(near, "pipe", 1)], axis=0)

    def to_or_from_relative(value):
        value = value.reshape(n_pipe, n_mp, rows)
        return flip_by(flip_by(value, 0, pipe, n_pipe), 1, mp, n_mp).reshape(-1)

    logits = lax.dot_general(
        everyone, unembedding, (((1,), (1,)), ((), ())), preferred_element_type=f32
    )
    vocab_start = lax.axis_index(("pipe", "mp")) * unembedding.shape[0]
    local_ids = to_or_from_relative(target_ids) - vocab_start
    columns = lax.broadcasted_iota(jnp.int32, logits.shape, 1)
    picked = jnp.sum(jnp.where(columns == local_ids[:, None], logits, 0.0), axis=1)
    top = jnp.max(logits, axis=1)
    exps = jnp.sum(jnp.exp(logits - top[:, None]), axis=1)
    stats = jnp.stack([to_or_from_relative(v) for v in (top, exps, picked)])
    every_stats = jnp.stack([swap(stats, ("pipe", "mp"), k) for k in range(n_pipe * n_mp)])
    top_all = jnp.max(every_stats[:, 0], axis=0)
    exp_total = jnp.sum(every_stats[:, 1] * jnp.exp(every_stats[:, 0] - top_all), axis=0)
    picked_all = jnp.sum(every_stats[:, 2], axis=0)
    token_logps = (picked_all - top_all - jnp.log(exp_total)).reshape(seq_count, length)

    divisor = counts / n_dp
    policy = jnp.sum(mask_values * token_logps, axis=1) / divisor
    anchor = jnp.sum(mask_values * anchor_logps, axis=1) / divisor
    log_gaps = policy - anchor
    positions = jnp.arange(seq_count, dtype=jnp.int32)
    chosen = jnp.sum(
        jnp.where(pairing[0, 0::2][:, None] == positions[None, :], log_gaps[None, :], 0.0), axis=1
    )
    rejected = jnp.sum(
        jnp.where(pairing[0, 1::2][:, None] == positions[None, :], log_gaps[None, :], 0.0), axis=1
    )
    losses = (chosen - rejected - 0.5 / ipo_tau) ** 2
    return (token_logps, policy, losses)


def solution(mesh):
    return jax.shard_map(
        shards,
        mesh=mesh,
        in_specs=(
            P("dp", None, None),
            P("pipe", "dp", "mp"),
            P("pipe", "mp", "dp"),
            P("pipe", None),
            P(),
            P(("pipe", "mp"), None),
            P("dp", None),
            P("dp", None),
            P("dp", None),
            P("dp", None),
        ),
        out_specs=(P("dp", None), P("dp"), P("dp")),
        check_vma=False,
    )
```

```python
import jax
import jax.numpy as jnp
from jax import lax
from jax.sharding import PartitionSpec as P


epsilon = 1e-05
ipo_tau = 0.5


def shift(value, axis, steps):
    count = lax.axis_size(axis)
    if steps % count == 0:
        return value
    return lax.ppermute(value, axis, [(i, (i + steps) % count) for i in range(count)])


def swap(value, axis, mask):
    if mask == 0:
        return value
    count = lax.axis_size(axis)
    return lax.ppermute(value, axis, [(i, i ^ mask) for i in range(count)])


def flip_by(value, axis, index, count):
    bit = 1
    while bit < count:
        shape = value.shape
        parts = value.reshape(shape[:axis] + (count // (2 * bit), 2, bit) + shape[axis + 1 :])
        turned = jnp.flip(parts, axis + 1)
        value = jnp.where((index & bit) != 0, turned, parts).reshape(shape)
        bit *= 2
    return value


def shards_body(
    hidden_states,
    up_weight,
    down_weight,
    layer_gain,
    final_gain,
    unembedding,
    target_ids,
    response_masks,
    anchor_logps,
    pairing,
):
    seq_count, length, width = hidden_states.shape
    n_dp, n_mp, n_pipe = lax.axis_size("dp"), lax.axis_size("mp"), lax.axis_size("pipe")
    dp, mp, pipe = lax.axis_index("dp"), lax.axis_index("mp"), lax.axis_index("pipe")
    rows = seq_count * length // (n_pipe * n_mp)
    cols = up_weight.shape[1]
    f32, bf16 = jnp.float32, jnp.bfloat16

    mask_values = response_masks.astype(f32)
    local_counts = jnp.sum(mask_values, axis=1)
    counts = local_counts
    for step in range(1, n_dp):
        counts = counts + shift(local_counts, "dp", step)

    def both(own):
        other = swap(own, "pipe", 1)
        first = jnp.where(pipe == 0, own, other)
        second = jnp.where(pipe == 0, other, own)
        return first, second

    gain_own = lax.dynamic_slice_in_dim(layer_gain[0], dp * cols, cols, 0)
    ups = lax.optimization_barrier(both(up_weight[0]))
    downs = lax.optimization_barrier(both(down_weight[0]))
    gains = both(gain_own)

    x_core = lax.dynamic_index_in_dim(
        hidden_states.reshape(n_pipe, n_mp, rows, width), pipe, 0, keepdims=False
    )
    x_mine = lax.dynamic_index_in_dim(x_core, mp, 0, keepdims=False)
    x_wide = x_core.astype(f32)
    mean_square = jnp.mean(x_wide * x_wide, axis=-1)
    row_scale = flip_by(lax.rsqrt(mean_square + epsilon), 0, mp, n_mp).reshape(-1)

    blocks = []
    for step in range(n_dp):
        start = ((dp + step) % n_dp) * cols
        blocks.append(shift(lax.dynamic_slice_in_dim(x_mine, start, cols, 1), "dp", step))

    def gather_mp(block):
        return jnp.concatenate([swap(block, "mp", k) for k in range(n_mp)], axis=0)

    def gather_group(members, found):
        joined = jnp.concatenate([blocks[t] for t in members], axis=0)
        pieces = [swap(joined, "mp", k) for k in range(n_mp)]
        for place, t in enumerate(members):
            found[t] = jnp.concatenate(
                [piece[place * rows : (place + 1) * rows] for piece in pieces], axis=0
            )

    order = list(range(1, n_dp)) + [0]
    late_groups = [[t] for t in range(n_dp)]

    def section(blocks, gathered, row_scale, gain, up, down):
        partials, squares = {}, {}
        for t in order:
            wide = gathered[t].astype(f32)
            scaled = (wide * gain).astype(bf16)
            whole = lax.optimization_barrier(jnp.dot(scaled, up, preferred_element_type=f32))
            partials[t] = jnp.split(whole, 1, axis=1)
            squares[t] = jnp.sum(wide * wide, axis=-1)
        totals = partials[order[0]]
        square_sum = squares[order[0]]
        for t in order[1:]:
            totals = [
                shift(total.astype(bf16), "dp", 1).astype(f32) + partial
                for total, partial in zip(totals, partials[t])
            ]
            if row_scale is None:
                square_sum = shift(square_sum, "dp", 1) + squares[t]
        if row_scale is None:
            row_scale = lax.rsqrt(square_sum / width + epsilon)
        current = [jax.nn.silu(total * row_scale[:, None]).astype(bf16) for total in totals]
        results = {}
        for group in late_groups:
            outs = []
            for t in group:
                if t > 0:
                    current = [shift(piece, "dp", 1) for piece in current]
                active = jnp.concatenate(current, axis=1)
                out = jnp.dot(active, down, preferred_element_type=f32)
                outs.append(out.reshape(n_mp, rows, cols))
            summed = jnp.concatenate([blocks[t].astype(f32) + out[0] for t, out in zip(group, outs)])
            for k in range(1, n_mp):
                sent = jnp.concatenate([out[k].astype(bf16) for out in outs])
                got = swap(sent, "mp", k)
                summed = summed + got.astype(f32)
            summed = summed.astype(bf16)
            for place, t in enumerate(group):
                results[t] = summed[place * rows : (place + 1) * rows]
        return results

    gathered = {}
    for group in [[t] for t in order]:
        gather_group(group, gathered)
    gathered[order[-1]], counts = lax.optimization_barrier((gathered[order[-1]], counts))
    blocks = section(blocks, gathered, row_scale, gains[0], ups[0], downs[0])
    gathered = {}
    for group in late_groups:
        gather_group(group, gathered)
    blocks = section(blocks, gathered, None, gains[1], ups[1], downs[1])

    home = [shift(blocks[t], "dp", -t) for t in range(n_dp)]
    doubled = jnp.concatenate([jnp.stack(home), jnp.stack(home)], axis=0)
    placed = lax.dynamic_slice_in_dim(doubled, (n_dp - dp) % n_dp, n_dp, 0)
    finals = jnp.transpose(placed, (1, 0, 2)).reshape(rows, width).astype(f32)
    mean_square = jnp.mean(finals * finals, axis=-1, keepdims=True)
    normed = (finals * lax.rsqrt(mean_square + epsilon) * final_gain).astype(bf16)
    near = gather_mp(normed)
    everyone = jnp.concatenate([near, swap(near, "pipe", 1)], axis=0)

    def to_or_from_relative(value):
        value = value.reshape(n_pipe, n_mp, rows)
        return flip_by(flip_by(value, 0, pipe, n_pipe), 1, mp, n_mp).reshape(-1)

    logits = lax.dot_general(
        everyone, unembedding, (((1,), (1,)), ((), ())), preferred_element_type=f32
    )
    vocab_start = lax.axis_index(("pipe", "mp")) * unembedding.shape[0]
    local_ids = to_or_from_relative(target_ids) - vocab_start
    columns = lax.broadcasted_iota(jnp.int32, logits.shape, 1)
    picked = jnp.sum(jnp.where(columns == local_ids[:, None], logits, 0.0), axis=1)
    top = jnp.max(logits, axis=1)
    exps = jnp.sum(jnp.exp(logits - top[:, None]), axis=1)
    stats = jnp.stack([to_or_from_relative(v) for v in (top, exps, picked)])
    for axis, count in (("mp", n_mp), ("pipe", n_pipe)):
        several = jnp.stack([swap(stats, axis, k) for k in range(count)])
        top_all = jnp.max(several[:, 0], axis=0)
        exp_total = jnp.sum(several[:, 1] * jnp.exp(several[:, 0] - top_all), axis=0)
        picked_all = jnp.sum(several[:, 2], axis=0)
        stats = jnp.stack([top_all, exp_total, picked_all])
    token_logps = (picked_all - top_all - jnp.log(exp_total)).reshape(seq_count, length)

    divisor = counts / n_dp
    policy = jnp.sum(mask_values * token_logps, axis=1) / divisor
    anchor = jnp.sum(mask_values * anchor_logps, axis=1) / divisor
    log_gaps = policy - anchor
    positions = jnp.arange(seq_count, dtype=jnp.int32)
    chosen = jnp.sum(
        jnp.where(pairing[0, 0::2][:, None] == positions[None, :], log_gaps[None, :], 0.0), axis=1
    )
    rejected = jnp.sum(
        jnp.where(pairing[0, 1::2][:, None] == positions[None, :], log_gaps[None, :], 0.0), axis=1
    )
    losses = (chosen - rejected - 0.5 / ipo_tau) ** 2
    return (token_logps, policy, losses)


def solution(mesh):
    return jax.shard_map(
        shards_body,
        mesh=mesh,
        in_specs=(
            P("dp", None, None),
            P("pipe", "dp", "mp"),
            P("pipe", "mp", "dp"),
            P("pipe", None),
            P(),
            P(("pipe", "mp"), None),
            P("dp", None),
            P("dp", None),
            P("dp", None),
            P("dp", None),
        ),
        out_specs=(P("dp", None), P("dp"), P("dp")),
        check_vma=False,
    )
```
